32 devices in a mesh: groups: 2 (over y), tensor: 4 (over z), seq: 4 (over x, core).
Axes of the slice: x: 2, y: 2, z: 4, core: 2. Of those that a mesh axis runs over, the one named last changes fastest.
Arguments:
- stream: bfloat16 [2048, 4096], P(('groups', 'seq'), 'tensor'), parts along dimension 0, may hold values from -150 to 150, as said below
- ffn_gain: float32 [4096], replicated, may hold values from 0.5 to 1.5
- final_gain: float32 [4096], replicated, may hold values from 0.5 to 1.5
- w_gate: bfloat16 [4096, 5120], P(None, 'tensor'), may hold values from -0.09375 to 0.09375
- w_up: bfloat16 [4096, 5120], P(None, 'tensor'), may hold values from -0.09375 to 0.09375
- w_out: bfloat16 [5120, 4096], P('tensor'), may hold values from -0.25 to 0.25
- w_key: bfloat16 [4096, 2048], P(None, 'tensor'), may hold values from -0.09375 to 0.09375
- w_value: bfloat16 [4096, 2048], P(None, 'tensor'), may hold values from -0.09375 to 0.09375
Outputs:
- enc_out: bfloat16 [2048, 4096], P(('groups', 'seq'), 'tensor'), parts along dimension 0
- cross_keys: bfloat16 [2048, 2048], P('groups', 'tensor'), parts along dimension 0
- cross_values: bfloat16 [2048, 2048], P('groups', 'tensor'), parts along dimension 0
The draws below stay inside these ranges and needn't reach their ends.
There are 2 independent parts, one for each index of `groups`. The reference program is written for one: setup_inputs(seed, part) draws one part's arguments, and reference() takes and returns one part's arrays. A program takes and returns all parts, laid end to end along the dimension named above; an argument that names none is the same for every part. Nothing has to cross between parts.
Inputs may be any that keep to these rules, and one draw needn't show every extreme that they name: Finite entries of the residual stream.
All inputs are finite; a program needn't handle non-finite values.
Results may differ from the reference program's by a relative error of at most 0.0055.
Values may be sent and summed in bfloat16 or wider, within the bound.
No kernel may reach another device: no remote copies, remote signals or barrier semaphores. Data moves between devices by JAX's collectives and lax.ppermute only.
A program may use at most 128 MiB of HBM per device.

```python
import jax
import jax.numpy as jnp
from jax import lax

D = 4096
FF = 5120
TOKENS = 1024
KV_WIDTH = 2048


def draw_stream(key, part):
    key_base = jax.random.fold_in(key, 11)
    key_rows = jax.random.fold_in(key, 12)
    key_cols = jax.random.fold_in(key, 13)
    row_scale = jnp.exp(jax.random.uniform(key_rows, (TOKENS, 1), jnp.float32, jnp.log(0.3), jnp.log(3.0)))
    rising = 3.0 ** (jnp.arange(D, dtype=jnp.float32) / D)
    col_scale = rising[None, :] * jnp.exp(jax.random.uniform(key_cols, (1, D), jnp.float32, 0.0, jnp.log(3.3)))
    base_vals = jax.random.normal(key_base, (TOKENS, D), jnp.float32)
    base_vals = jnp.clip(base_vals, -5.0, 5.0)
    return (base_vals * row_scale * col_scale).astype(jnp.bfloat16)


def strengthened(drawn, own_key, source, target, shards_of, factor):
    def block_of(dim):
        return (jnp.arange(drawn.shape[dim]) // (drawn.shape[dim] // shards_of)).reshape((-1,) + (1,) * (drawn.ndim - 1 - dim))

    one_side = jax.random.permutation(own_key, shards_of)[block_of(target)]
    second = (block_of(target) + shards_of // 2) % shards_of
    return jnp.where((block_of(source) == one_side) | (block_of(source) == second), factor * drawn, drawn)


def shard_levels(key, dims, split, least, largest):
    loudness = 1.0
    for dim, parts in split:
        steps = jax.random.uniform(jax.random.fold_in(jax.random.fold_in(key, 6), dim), (parts,), jnp.float32, least / len(split), largest / len(split))
        loudness = loudness * jnp.repeat(jnp.exp(steps), dims[dim] // parts).reshape((-1,) + (1,) * (len(dims) - 1 - dim))
    return loudness


def gaussian(stream_key, shape, deviation, most, cuts=(), held_as=jnp.bfloat16):
    loudness = shard_levels(stream_key, shape, cuts, -0.22, 0.18) if cuts else 1.0
    drawn = jax.random.normal(stream_key, shape, jnp.float32) * deviation * loudness
    return jnp.minimum(jnp.maximum(drawn, -most), most).astype(held_as)


def noise_with(key, extent, scale, bound, cuts, heavy, held_as=jnp.bfloat16):
    values = scale * jax.random.normal(key, extent, jnp.float32)
    if cuts:
        values = values * shard_levels(key, extent, cuts, -0.22, 0.18)
    return jnp.clip(strengthened(values, jax.random.fold_in(key, 3), *heavy), -bound, bound).astype(held_as)


def setup_inputs(seed: int = 0, part: int = 0) -> dict:
    key_list = jax.random.split(jax.random.key(seed), 9)
    own_keys = jax.random.split(jax.random.fold_in(key_list[8], part), 9)
    return {
        "stream": draw_stream(jax.random.fold_in(jax.random.fold_in(key_list[8], part), 71), part),
        "ffn_gain": jnp.clip(1.0 + 0.1 * jax.random.normal(key_list[1], (D,), jnp.float32), 0.5, 1.5),
        "final_gain": jnp.clip(1.0 + 0.1 * jax.random.normal(key_list[2], (D,), jnp.float32), 0.5, 1.5),
        "w_gate": gaussian(key_list[3], (D, FF), D ** -0.5, 0.09375, ((1, 4),)),
        "w_up": gaussian(key_list[4], (D, FF), D ** -0.5, 0.09375, ((1, 4),)),
        "w_out": noise_with(key_list[5], (FF, D), (FF // 4) ** -0.5, 0.25, ((0, 4),), (0, 1, 4, 2.0)),
        "w_key": gaussian(key_list[6], (D, KV_WIDTH), D ** -0.5, 0.09375, ((1, 4),)),
        "w_value": gaussian(key_list[7], (D, KV_WIDTH), D ** -0.5, 0.09375, ((1, 4),)),
    }


epsilon = 1e-06

def rms_norm(vector, gain):
    return vector * lax.rsqrt(lax.optimization_barrier(jnp.mean(vector * vector, axis=-1, keepdims=True)) + epsilon) * gain

def reference(stream, ffn_gain, final_gain, w_gate, w_up, w_out, w_key, w_value):
    stream_wide = stream.astype(jnp.float32)
    normed_in = rms_norm(stream_wide, ffn_gain).astype(jnp.bfloat16)
    gate_act = jnp.dot(normed_in, w_gate, preferred_element_type=jnp.float32)
    up_proj = jnp.dot(normed_in, w_up, preferred_element_type=jnp.float32)
    hidden = (jax.nn.gelu(gate_act, approximate=True) * up_proj).astype(jnp.bfloat16)
    mixed = stream_wide + jnp.dot(hidden, w_out, preferred_element_type=jnp.float32)
    enc_out = rms_norm(mixed, final_gain).astype(jnp.bfloat16)
    cross_keys = jnp.dot(enc_out, w_key, preferred_element_type=jnp.float32).astype(jnp.bfloat16)
    cross_values = jnp.dot(enc_out, w_value, preferred_element_type=jnp.float32).astype(jnp.bfloat16)
    return (enc_out, cross_keys, cross_values)
```

```python
import jax
import jax.numpy as jnp
from jax import lax
from jax.experimental import pallas as pl
from jax.experimental.pallas import tpu as pltpu
from jax.sharding import PartitionSpec as P

epsilon = 1e-06
CHUNKS = 2


def swap(value, axis, distance):
    size = lax.axis_size(axis)
    return lax.ppermute(value, axis, [(i, i ^ distance) for i in range(size)])


def distances(size):
    d = size // 2
    while d:
        yield d
        d //= 2


def gathered(own, axis):
    have = {0: own}
    for d in distances(lax.axis_size(axis)):
        for r in sorted(have, reverse=True):
            have[r ^ d] = swap(have[r], axis, d)
    return [have[r] for r in range(len(have))]


def relative(axis):
    return lax.axis_index(axis) ^ jnp.arange(lax.axis_size(axis), dtype=jnp.int32)


def tile_of(size, most):
    tile = most
    while tile >= 128:
        if size % tile == 0:
            return tile
        tile -= 128
    return size


def ffn_kernel(n, hid_steps, order, *refs):
    blocks = refs[:n]
    gain, w_gate, w_up, w_out, send, keep, normed, hidden, own_rows = refs[n:]
    step = pl.program_id(0)
    tokens, feats = blocks[0].shape
    rows = tokens // n
    hid_tile = w_gate.shape[1]
    out_tile = w_out.shape[1]

    @pl.when(step == 0)
    def _():
        for r in range(n):
            span = pl.ds(pl.multiple_of(order[r] * rows, rows), rows)
            total = jnp.zeros((rows, 1), jnp.float32)
            for b in range(n):
                wide = blocks[b][span, :].astype(jnp.float32)
                total += jnp.sum(wide * wide, axis=1, keepdims=True)
            scale = lax.rsqrt(total / (n * feats) + epsilon)
            for b in range(n):
                wide = blocks[b][span, :].astype(jnp.float32)
                cols = pl.ds(pl.multiple_of(order[b] * feats, feats), feats)
                normed[r * rows:(r + 1) * rows, cols] = (wide * scale * gain[:, cols]).astype(jnp.bfloat16)
                if r == 0:
                    own_rows[:, cols] = wide

    @pl.when(step < hid_steps)
    def _():
        gate_act = jnp.dot(normed[...], w_gate[...], preferred_element_type=jnp.float32)
        up_proj = jnp.dot(normed[...], w_up[...], preferred_element_type=jnp.float32)
        hidden[step] = (jax.nn.gelu(gate_act, approximate=True) * up_proj).astype(jnp.bfloat16)

    @pl.when(step >= hid_steps)
    def _():
        total = jnp.dot(hidden[0], w_out[:hid_tile, :], preferred_element_type=jnp.float32)
        for s in range(1, hid_steps):
            total += jnp.dot(hidden[s], w_out[s * hid_tile:(s + 1) * hid_tile, :], preferred_element_type=jnp.float32)
        cols = pl.ds(pl.multiple_of((step - hid_steps) * out_tile, out_tile), out_tile)
        for r in range(n):
            part = total[r * rows:(r + 1) * rows, :]
            if r % 2:
                send[r // 2] = part.astype(jnp.bfloat16)
            elif r:
                keep[r // 2] = part
            else:
                keep[0] = part + own_rows[:, cols]


def ffn(order, blocks, gain, w_gate, w_up, w_out):
    n = len(blocks)
    tokens, feats = blocks[0].shape
    rows, width, units = tokens // n, n * feats, w_gate.shape[1]
    hid_tile, out_tile = tile_of(units, 256), tile_of(width, 512)
    hid_steps, out_steps = units // hid_tile, width // out_tile

    def whole(i, o):
        return (0, 0)

    def hid_at(i, o):
        return (0, jnp.minimum(i, hid_steps - 1))

    def out_at(i, o):
        return (0, jnp.maximum(i - hid_steps, 0))

    def res_at(i, o):
        return (0, 0, jnp.maximum(i - hid_steps, 0))

    return pl.pallas_call(
        lambda *a: ffn_kernel(n, hid_steps, *a),
        out_shape=(
            jax.ShapeDtypeStruct((n // 2, rows, width), jnp.bfloat16),
            jax.ShapeDtypeStruct((n // 2, rows, width), jnp.float32),
        ),
        grid_spec=pltpu.PrefetchScalarGridSpec(
            num_scalar_prefetch=1,
            grid=(hid_steps + out_steps,),
            in_specs=[pl.BlockSpec((tokens, feats), whole)] * n
            + [
                pl.BlockSpec((1, width), whole),
                pl.BlockSpec((width, hid_tile), hid_at),
                pl.BlockSpec((width, hid_tile), hid_at),
                pl.BlockSpec((units, out_tile), out_at),
            ],
            out_specs=[
                pl.BlockSpec((n // 2, rows, out_tile), res_at),
                pl.BlockSpec((n // 2, rows, out_tile), res_at),
            ],
            scratch_shapes=[
                pltpu.VMEM((tokens, width), jnp.bfloat16),
                pltpu.VMEM((hid_steps, tokens, hid_tile), jnp.bfloat16),
                pltpu.VMEM((rows, width), jnp.float32),
            ],
        ),
        compiler_params=pltpu.CompilerParams(dimension_semantics=("arbitrary",), vmem_limit_bytes=40 << 20),
        cost_estimate=pl.CostEstimate(
            flops=6 * tokens * width * units, bytes_accessed=6 * width * units, transcendentals=tokens * units
        ),
        name="ffn",
    )(order, *blocks, gain.reshape(1, -1), w_gate, w_up, w_out)


def final_kernel(base, extra, gain, out):
    mixed = base[...] + extra[...].astype(jnp.float32)
    mean = jnp.mean(mixed * mixed, axis=1, keepdims=True)
    out[...] = (mixed * lax.rsqrt(mean + epsilon) * gain[...]).astype(jnp.bfloat16)


def final_norm(base, extra, gain):
    rows, width = base.shape
    return pl.pallas_call(
        final_kernel,
        out_shape=jax.ShapeDtypeStruct((rows, width), jnp.bfloat16),
        cost_estimate=pl.CostEstimate(flops=8 * rows * width, bytes_accessed=8 * rows * width, transcendentals=rows),
        name="final_norm",
    )(base, extra, gain.reshape(1, -1))


def kv_kernel(n, order, *refs):
    blocks = refs[:n]
    w_key, w_value, enc_out, local_kv, ordered, keys, values = refs[n:]
    step, steps = pl.program_id(0), pl.num_programs(0)
    rows, width = blocks[0].shape
    feats = enc_out.shape[1]
    depth = w_key.shape[0]
    kv_cols = w_key.shape[1]

    @pl.when(step == 0)
    def _():
        for r in range(n):
            span = pl.ds(pl.multiple_of(order[r] * rows, rows), rows)
            ordered[span, :] = blocks[r][...]
        keys[...] = jnp.zeros_like(keys)
        values[...] = jnp.zeros_like(values)
        enc_out[...] = ordered[:, pl.ds(pl.multiple_of(order[0] * feats, feats), feats)]

    part = ordered[:, pl.ds(pl.multiple_of(step * depth, depth), depth)]
    keys[...] += jnp.dot(part, w_key[...], preferred_element_type=jnp.float32)
    values[...] += jnp.dot(part, w_value[...], preferred_element_type=jnp.float32)

    @pl.when(step == steps - 1)
    def _():
        local_kv[:, :kv_cols] = keys[...].astype(jnp.bfloat16)
        local_kv[:, kv_cols:] = values[...].astype(jnp.bfloat16)


def project(order, blocks, w_key, w_value):
    n = len(blocks)
    rows, width = blocks[0].shape
    kv_cols = w_key.shape[1]
    depth = tile_of(width, 1024)
    return pl.pallas_call(
        lambda *a: kv_kernel(n, *a),
        out_shape=(
            jax.ShapeDtypeStruct((n * rows, width // n), jnp.bfloat16),
            jax.ShapeDtypeStruct((n * rows, 2 * kv_cols), jnp.bfloat16),
        ),
        grid_spec=pltpu.PrefetchScalarGridSpec(
            num_scalar_prefetch=1,
            grid=(width // depth,),
            in_specs=[pl.BlockSpec((rows, width), lambda i, o: (0, 0))] * n
            + [pl.BlockSpec((depth, kv_cols), lambda i, o: (i, 0))] * 2,
            out_specs=[
                pl.BlockSpec((n * rows, width // n), lambda i, o: (0, 0)),
                pl.BlockSpec((n * rows, 2 * kv_cols), lambda i, o: (0, 0)),
            ],
            scratch_shapes=[
                pltpu.VMEM((n * rows, width), jnp.bfloat16),
                pltpu.VMEM((n * rows, kv_cols), jnp.float32),
                pltpu.VMEM((n * rows, kv_cols), jnp.float32),
            ],
        ),
        compiler_params=pltpu.CompilerParams(dimension_semantics=("arbitrary",)),
        cost_estimate=pl.CostEstimate(
            flops=4 * n * rows * width * kv_cols, bytes_accessed=4 * width * kv_cols, transcendentals=0
        ),
        name="project",
    )(order, *blocks, w_key, w_value)


def place_kernel(count, chunks, order, *refs):
    pieces = refs[: count * chunks]
    keys, values = refs[count * chunks:]
    kv_cols = keys.shape[-1]
    for c in range(chunks):
        for r in range(count):
            piece = pieces[c * count + r]
            keys[order[r], c] = piece[:, :kv_cols]
            values[order[r], c] = piece[:, kv_cols:]


def place(order, pieces):
    chunks, count = len(pieces), len(pieces[0])
    tokens, both = pieces[0][0].shape
    shape = (count, chunks, tokens, both // 2)
    flat = [p for chunk in pieces for p in chunk]
    keys, values = pl.pallas_call(
        lambda *a: place_kernel(count, chunks, *a),
        out_shape=(jax.ShapeDtypeStruct(shape, jnp.bfloat16),) * 2,
        in_specs=[pl.BlockSpec(memory_space=pltpu.SMEM)] + [pl.BlockSpec(memory_space=pltpu.VMEM)] * len(flat),
        cost_estimate=pl.CostEstimate(flops=0, bytes_accessed=8 * tokens * both * len(flat) // 2, transcendentals=0),
        name="place",
    )(order, *flat)
    return keys.reshape(-1, both // 2), values.reshape(-1, both // 2)


def on_device(stream, ffn_gain, final_gain, w_gate, w_up, w_out, w_key, w_value):
    n = lax.axis_size("tensor")
    order = relative("tensor")
    seq_order = relative("seq")
    tokens = stream.shape[0] // CHUNKS
    encoded, pieces = [], []
    for c in range(CHUNKS):
        blocks = gathered(stream[c * tokens:(c + 1) * tokens], "tensor")
        send, keep = ffn(order, blocks, ffn_gain, w_gate, w_up, w_out)
        d = 1
        while True:
            received = swap(send, "tensor", d)
            d *= 2
            if d == n:
                break
            total = keep + received.astype(jnp.float32)
            total = total.reshape((-1, 2) + total.shape[1:])
            send, keep = total[:, 1].astype(jnp.bfloat16), total[:, 0]
        rows = final_norm(keep[0], received[0], final_gain)
        enc, kv = project(order, gathered(rows, "tensor"), w_key, w_value)
        encoded.append(enc)
        pieces.append(gathered(kv, "seq"))
    keys, values = place(seq_order, pieces)
    return jnp.concatenate(encoded, axis=0), keys, values


def solution(mesh):
    placed = (
        P(("groups", "seq"), "tensor"),
        P(),
        P(),
        P(None, "tensor"),
        P(None, "tensor"),
        P("tensor", None),
        P(None, "tensor"),
        P(None, "tensor"),
    )
    return jax.shard_map(
        on_device,
        mesh=mesh,
        in_specs=placed,
        out_specs=(P(("groups", "seq"), "tensor"), P("groups", "tensor"), P("groups", "tensor")),
        check_vma=False,
    )
```
